32 devices in a mesh: grp: 2 (over x), rep: 4 (over z), tp: 4 (over y, core).
Axes of the slice: x: 2, y: 2, z: 4, core: 2. Of those that a mesh axis runs over, the one named last changes fastest.
Arguments:
- grad_parts: float32 [4, 5120, 2048], P('tp', ('grp', 'rep')), may hold values from -124 to 124
- master: float32 [5120, 2048], P(('grp', 'rep'), 'tp'), may hold values from -0.078125 to 0.078125
- moment_one: float32 [5120, 2048], P(('grp', 'rep'), 'tp'), may hold values from -1.5 to 1.5
- moment_two: float32 [5120, 2048], P(('grp', 'rep'), 'tp'), may hold values from 0.003 to 0.03
- hidden_in: bfloat16 [32, 4, 5120], P(('grp', 'rep')), may hold values from -6 to 6
- queries: bfloat16 [32, 4, 5120], P(('grp', 'rep'), None, 'tp'), may hold values from -8 to 8
- cache_keys: bfloat16 [32, 1024, 1024], P(('grp', 'rep'), None, 'tp'), may hold values from -8 to 8
- cache_values: bfloat16 [32, 1024, 1024], P(('grp', 'rep'), None, 'tp'), may hold values from -6 to 6
- cache_lengths: int32 [32], P(('grp', 'rep')), may hold values from 16 to 1024
Outputs:
- new_moment_one: float32 [5120, 2048], P(('grp', 'rep'), 'tp')
- new_moment_two: float32 [5120, 2048], P(('grp', 'rep'), 'tp')
- new_entries: bfloat16 [32, 4, 2048], P(('grp', 'rep'), None, 'tp')
- attended: bfloat16 [32, 4, 5120], P(('grp', 'rep'), None, 'tp')
The draws below stay inside these ranges and needn't reach their ends.
Inputs may be any that keep to these rules, and one draw needn't show every extreme that they name: `cache_lengths`: cache slots at or after a row's length hold no part of its cache.
All inputs are finite; a program needn't handle non-finite values.
Results may differ from the reference program's by a relative error of at most 0.0051.
Values may be sent and summed in bfloat16 or wider, within the bound.
A program may use at most 64 MiB of HBM per device.

```python
import math
import jax
import jax.numpy as jnp
from jax import lax

D = 5120
QH = 40
KVH = 8
HD = 128
CACHE = 1024
STEPS = 4
ROWS = 32
N_GRP = 2
N_REP = 4
N_TP = 4


def grad_levels(key):
    block_rows = D // (N_GRP * N_REP)
    row_power = jax.random.uniform(jax.random.fold_in(key, 34), (N_GRP * N_REP,), jnp.float32, -0.5, 0.0)
    row_level = jnp.repeat(jnp.exp(math.log(10.0) * row_power), block_rows)
    col_power = jax.random.uniform(jax.random.fold_in(key, 35), (2 * KVH,), jnp.float32, -1.0, 0.0)
    col_level = jnp.repeat(jnp.exp(math.log(10.0) * col_power), HD)
    return row_level[None, :, None] * col_level[None, None, :]


def draw_grad_parts(key, part):
    data_index = jnp.arange(N_TP, dtype=jnp.float32)
    row_index = jnp.arange(D, dtype=jnp.float32)
    growth = (1.0 + 2.0 * data_index / (N_TP - 1))[:, None, None] * (1.0 + 2.0 * row_index / (D - 1))[None, :, None]
    growth = growth * grad_levels(key)
    shape = (N_TP, D, 2 * KVH * HD)
    noise = jax.random.truncated_normal(jax.random.fold_in(key, 33), -6.0, 6.0, shape, jnp.float32)
    return noise * growth


def draw_queries(key, part):
    shape = (ROWS, STEPS, QH * HD)
    return jax.random.truncated_normal(jax.random.fold_in(key, 42), -6.0, 6.0, shape, jnp.float32).astype(jnp.bfloat16)


def draw_cache_keys(key, part):
    shape = (ROWS, CACHE, KVH * HD)
    return jax.random.truncated_normal(jax.random.fold_in(key, 52), -6.0, 6.0, shape, jnp.float32).astype(jnp.bfloat16)


def plant(values, key, smallest, top_value):
    longest = values.shape.index(max(values.shape))
    spots = []
    for shift in (0, 1):
        where = [jax.random.randint(jax.random.fold_in(key, axis), (), 0, length) for axis, length in enumerate(values.shape)]
        where[longest] = (where[longest] + shift) % values.shape[longest]
        spots.append(tuple(where))
    return values.at[spots[0]].set(smallest).at[spots[1]].set(top_value)


def block_scale(stream_key, shape, cuts, least, largest):
    gain, own = 1.0, jax.random.fold_in(stream_key, 6)
    for position, parts in cuts:
        draws = jnp.exp(jax.random.uniform(jax.random.fold_in(own, position), (parts,), jnp.float32, least / len(cuts), largest / len(cuts)))
        gain = gain * jnp.repeat(draws, shape[position] // parts).reshape([-1 if axis == position else 1 for axis in range(len(shape))])
    return gain


def scatter_about(own_key, dims, scale, reach, pieces=(), held_as=jnp.bfloat16):
    entries = scale * jax.random.normal(own_key, dims, jnp.float32)
    if pieces:
        entries = entries * block_scale(own_key, dims, pieces, -0.22, 0.18)
    return jnp.clip(entries, -reach, reach).astype(held_as)


def setup_inputs(seed: int = 0) -> dict:
    splits = jax.random.split(jax.random.key(seed), 10)
    return {
        "grad_parts": draw_grad_parts(jax.random.fold_in(splits[9], 71), 0),
        "master": scatter_about(splits[1], (D, 2 * KVH * HD), D ** -0.5, 0.078125, ((0, 8), (1, 4)), jnp.float32),
        "moment_one": scatter_about(splits[2], (D, 2 * KVH * HD), 0.1, 1.5, ((0, 8), (1, 4)), jnp.float32),
        "moment_two": jnp.clip(jnp.exp(math.log(0.03) - 2.3025851 * jax.random.uniform(splits[3], (D, 2 * KVH * HD), jnp.float32) ** block_scale(splits[3], (D, 2 * KVH * HD), ((0, 8), (1, 4)), -0.2, 0.2)), 0.003, 0.03),
        "hidden_in": scatter_about(splits[4], (ROWS, STEPS, D), 1.0, 6.0, ((0, 8),)),
        "queries": draw_queries(jax.random.fold_in(splits[9], 71), 0),
        "cache_keys": draw_cache_keys(jax.random.fold_in(splits[9], 71), 0),
        "cache_values": scatter_about(splits[7], (ROWS, CACHE, KVH * HD), 1.0, 6.0, ((0, 8), (2, 4))),
        "cache_lengths": plant(jax.random.randint(splits[8], (ROWS,), 16, CACHE + 1), jax.random.fold_in(splits[8], 1), 16, CACHE).astype(jnp.int32),
    }


BETA_ONE = 0.9
BETA_TWO = 0.999
FIRST_CORR = 0.9999734386011124
SECOND_CORR = 0.09520785288629041
LEARN_RATE = 0.003
EPSILON = 1e-08
ROPE_BASE = 1000000.0
NEG_FILL = -1e+30

def rotate(new_keys, lengths):
    positions = (lengths[:, None] + jnp.arange(new_keys.shape[1], dtype=jnp.int32)[None, :]).astype(jnp.float32)
    half_dim = new_keys.shape[-1] // 2
    inverse = jnp.exp(-math.log(ROPE_BASE) * 2.0 * jnp.arange(half_dim, dtype=jnp.float32) / new_keys.shape[-1])
    angles = positions[:, :, None] * inverse[None, None, :]
    cosine_part = jnp.concatenate([jnp.cos(angles), jnp.cos(angles)], -1)[:, :, None, :]
    sine_part = jnp.concatenate([jnp.sin(angles), jnp.sin(angles)], -1)[:, :, None, :]
    rotated = jnp.concatenate([-new_keys[..., half_dim:], new_keys[..., :half_dim]], -1)
    return new_keys * cosine_part + rotated * sine_part

def attend_row(items):
    query_row, old_keys, old_values, length, new_keys, new_values = items
    groups = QH // KVH
    query_heads = query_row.reshape(STEPS, KVH, groups, HD).astype(jnp.float32)
    old_k = old_keys.reshape(CACHE, KVH, HD).astype(jnp.float32)
    old_v = old_values.reshape(CACHE, KVH, HD).astype(jnp.float32)
    scaling = 1.0 / math.sqrt(HD)
    old_scores = jnp.einsum('sagd,jad->sagj', query_heads, old_k) * scaling
    valid_slots = jnp.arange(CACHE, dtype=jnp.int32) < length
    old_scores = jnp.where(valid_slots[None, None, None, :], old_scores, NEG_FILL)
    new_scores = jnp.einsum('sagd,tad->sagt', query_heads, new_keys.astype(jnp.float32)) * scaling
    causal = jnp.arange(STEPS)[:, None] >= jnp.arange(STEPS)[None, :]
    new_scores = jnp.where(causal[:, None, None, :], new_scores, NEG_FILL)
    scores = jnp.concatenate([old_scores, new_scores], -1)
    row_max = lax.optimization_barrier(jnp.max(scores, -1, keepdims=True))
    exp_scores = jnp.exp(scores - row_max)
    probs = (exp_scores / lax.optimization_barrier(jnp.sum(exp_scores, -1, keepdims=True))).astype(jnp.bfloat16)
    output = jnp.einsum('sagj,jad->sagd', probs[..., :CACHE].astype(jnp.float32), old_v)
    output = output + jnp.einsum('sagt,tad->sagd', probs[..., CACHE:].astype(jnp.float32), new_values.astype(jnp.float32))
    return output.reshape(STEPS, QH * HD).astype(jnp.bfloat16)

def reference(grad_parts, master, moment_one, moment_two, hidden_in, queries, cache_keys, cache_values, cache_lengths):
    grad_sum = lax.optimization_barrier(jnp.sum(grad_parts, axis=0))
    squares = jnp.sum(grad_sum * grad_sum)
    norm_limit = math.sqrt(D * 2 * KVH * HD)
    clipped = grad_sum * jnp.minimum(1.0, norm_limit / jnp.sqrt(squares))
    new_moment_one = BETA_ONE * moment_one + (1.0 - BETA_ONE) * clipped
    new_moment_two = BETA_TWO * moment_two + (1.0 - BETA_TWO) * clipped * clipped
    update = new_moment_one / FIRST_CORR / (jnp.sqrt(new_moment_two / SECOND_CORR) + EPSILON)
    weights = (master - LEARN_RATE * update).astype(jnp.bfloat16)
    projected = jnp.dot(hidden_in.reshape(ROWS * STEPS, D), weights, preferred_element_type=jnp.float32)
    projected = projected.reshape(ROWS, STEPS, KVH, 2, HD)
    new_keys = rotate(projected[:, :, :, 0, :], cache_lengths).astype(jnp.bfloat16)
    new_values = projected[:, :, :, 1, :].astype(jnp.bfloat16)
    new_entries = jnp.stack([new_keys, new_values], 3).reshape(ROWS, STEPS, 2 * KVH * HD)
    attended = lax.map(attend_row, (queries, cache_keys, cache_values, cache_lengths, new_keys, new_values))
    return (new_moment_one, new_moment_two, new_entries, attended)
```

```python
import functools
import math

import jax
import jax.numpy as jnp
from jax import lax
from jax.experimental import pallas as pl
from jax.experimental.pallas import tpu as pltpu
from jax.sharding import PartitionSpec as P

D = 5120
QH = 40
KVH = 8
HD = 128


BETA_ONE = 0.9
BETA_TWO = 0.999
FIRST_CORR = 0.9999734386011124
SECOND_CORR = 0.09520785288629041
LEARN_RATE = 0.003
EPSILON = 1e-08
ROPE_BASE = 1000000.0
NEG_FILL = -1e30


def rotate(new_keys, lengths):
    positions = (lengths[:, None] + jnp.arange(new_keys.shape[1], dtype=jnp.int32)[None, :]).astype(
        jnp.float32
    )
    half_dim = new_keys.shape[-1] // 2
    inverse = jnp.exp(
        -math.log(ROPE_BASE) * 2.0 * jnp.arange(half_dim, dtype=jnp.float32) / new_keys.shape[-1]
    )
    angles = positions[:, :, None] * inverse[None, None, :]
    cosine_part = jnp.concatenate([jnp.cos(angles), jnp.cos(angles)], -1)[:, :, None, :]
    sine_part = jnp.concatenate([jnp.sin(angles), jnp.sin(angles)], -1)[:, :, None, :]
    rotated = jnp.concatenate([-new_keys[..., half_dim:], new_keys[..., :half_dim]], -1)
    return new_keys * cosine_part + rotated * sine_part


def body(
    grad_parts,
    master,
    moment_one,
    moment_two,
    hidden_in,
    queries,
    cache_keys,
    cache_values,
    cache_lengths,
):
    col_width = master.shape[1]
    grad_sum = lax.psum_scatter(grad_parts[0], "tp", scatter_dimension=1, tiled=True)
    squares = lax.psum(jnp.sum(grad_sum * grad_sum), ("grp", "rep", "tp"))
    norm_limit = math.sqrt(D * 2 * KVH * HD)
    clipped = grad_sum * jnp.minimum(1.0, norm_limit / jnp.sqrt(squares))
    new_moment_one = BETA_ONE * moment_one + (1.0 - BETA_ONE) * clipped
    new_moment_two = BETA_TWO * moment_two + (1.0 - BETA_TWO) * clipped * clipped
    update = new_moment_one / FIRST_CORR / (jnp.sqrt(new_moment_two / SECOND_CORR) + EPSILON)
    weights = (master - LEARN_RATE * update).astype(jnp.bfloat16)
    row_count, step_count, model_width = hidden_in.shape
    token_count = row_count * step_count
    flat_inputs = hidden_in.reshape(token_count, model_width)
    sliced = lax.all_to_all(
        lax.all_to_all(flat_inputs, "grp", split_axis=1, concat_axis=0, tiled=True),
        "rep",
        split_axis=1,
        concat_axis=0,
        tiled=True,
    )
    group_count = lax.axis_size("grp")
    replica_count = lax.axis_size("rep")
    ordered = sliced.reshape(replica_count, group_count, token_count, weights.shape[0])
    ordered = jnp.swapaxes(ordered, 0, 1).reshape(
        group_count * replica_count * token_count, weights.shape[0]
    )
    projected = lax.psum_scatter(
        jnp.dot(ordered, weights, preferred_element_type=jnp.float32),
        ("grp", "rep"),
        scatter_dimension=0,
        tiled=True,
    )
    heads_here = col_width // (2 * HD)
    projected = projected.reshape(row_count, step_count, heads_here, 2, HD)
    new_keys = rotate(projected[:, :, :, 0, :], cache_lengths).astype(jnp.bfloat16)
    new_values = projected[:, :, :, 1, :].astype(jnp.bfloat16)
    new_entries = jnp.stack([new_keys, new_values], 3).reshape(row_count, step_count, col_width)
    groups = QH // KVH
    slots = cache_keys.shape[1]
    query_heads = queries.reshape(row_count, step_count, heads_here, groups, HD)
    old_k = cache_keys.reshape(row_count, slots, heads_here, HD)
    old_v = cache_values.reshape(row_count, slots, heads_here, HD)
    scaling = 1.0 / math.sqrt(HD)
    old_scores = (
        jnp.einsum("rsagd,rjad->rsagj", query_heads, old_k, preferred_element_type=jnp.float32)
        * scaling
    )
    valid_slots = jnp.arange(slots, dtype=jnp.int32)[None, :] < cache_lengths[:, None]
    old_scores = jnp.where(valid_slots[:, None, None, None, :], old_scores, NEG_FILL)
    new_scores = (
        jnp.einsum("rsagd,rtad->rsagt", query_heads, new_keys, preferred_element_type=jnp.float32)
        * scaling
    )
    causal = jnp.arange(step_count)[:, None] >= jnp.arange(step_count)[None, :]
    new_scores = jnp.where(causal[None, :, None, None, :], new_scores, NEG_FILL)
    scores = jnp.concatenate([old_scores, new_scores], -1)
    row_max = jnp.max(scores, -1, keepdims=True)
    exp_scores = jnp.exp(scores - row_max)
    probs = (exp_scores / jnp.sum(exp_scores, -1, keepdims=True)).astype(jnp.bfloat16)
    output = jnp.einsum(
        "rsagj,rjad->rsagd", probs[..., :slots], old_v, preferred_element_type=jnp.float32
    )
    output = output + jnp.einsum(
        "rsagt,rtad->rsagd", probs[..., slots:], new_values, preferred_element_type=jnp.float32
    )
    attended = output.reshape(row_count, step_count, heads_here * groups * HD).astype(jnp.bfloat16)
    return (new_moment_one, new_moment_two, new_entries, attended)


MESH = pl.DeviceIdType.MESH
CHUNK = 64
PAD = 32


def fused_kernel(
    sizes,
    lengths_ref,
    cos_ref,
    sin_ref,
    hidden_ref,
    queries_ref,
    grad_ref,
    master_ref,
    one_ref,
    two_ref,
    keys_ref,
    values_ref,
    one_out,
    two_out,
    entries_out,
    attended_out,
    fwd_own,
    fwd_mate,
    sum_own,
    sum_mate,
    fwd_send,
    sum_far,
    grad_total,
    master_v,
    one_v,
    two_v,
    keys_v,
    values_v,
    hidden_in_v,
    hidden_f,
    weights_v,
    squares_send,
    squares_all,
    proj_send,
    proj_recv,
    query_f,
    old_max,
    old_sum,
    old_out,
    local_sem,
    mate_send_sem,
    mate_recv_sem,
    far_send_sem,
    far_recv_sem,
    hid_send_sem,
    hid_recv_sem,
    sq_send_sem,
    sq_recv_sem,
    proj_send_sem,
    proj_recv_sem,
    load_sem,
    cache_sem,
    out_sem,
):
    ngrp, nrep, ntp = sizes
    ngroup = ngrp * nrep
    ndev = ngroup * ntp
    rows, cols = master_ref.shape
    nrow, nstep, width = hidden_ref.shape
    tokens = nrow * nstep
    slots = keys_ref.shape[1]
    heads = cols // (2 * HD)
    groups = QH // KVH
    nchunk = rows // CHUNK
    scaling = 1.0 / math.sqrt(HD)

    g = lax.axis_index("grp")
    r = lax.axis_index("rep")
    t = lax.axis_index("tp")
    p = g * nrep + r
    flat = p * ntp + t
    y = t // 2
    c = t % 2
    mate = y * 2 + (1 - c)
    far = (1 - y) * 2 + c
    far_mate = (1 - y) * 2 + (1 - c)

    def flat_id(k):
        f = lax.rem(flat + k, ndev)
        q = f // ntp
        return {"grp": q // nrep, "rep": lax.rem(q, nrep), "tp": lax.rem(f, ntp)}

    def group_id(k):
        q = lax.rem(p + k, ngroup)
        return {"grp": q // nrep, "rep": lax.rem(q, nrep)}

    barrier = pltpu.get_barrier_semaphore()

    def greet(k, carry):
        pl.semaphore_signal(barrier, inc=1, device_id=flat_id(k), device_id_type=MESH)
        return carry

    lax.fori_loop(1, ndev, greet, 0)

    def block(i, owner):
        return grad_ref.at[0, pl.ds(pl.multiple_of(i * CHUNK, CHUNK), CHUNK), pl.ds(pl.multiple_of(owner * cols, cols), cols)]

    def at_rows(ref, i):
        return ref.at[pl.ds(pl.multiple_of(i * CHUNK, CHUNK), CHUNK)]

    def local_copy(which, i):
        owner, dst = ((far, fwd_own), (t, sum_own))[which]
        return pltpu.make_async_copy(block(i, owner), at_rows(dst, i), local_sem.at[which, i])

    def mate_copy(which, i):
        owner, dst = ((far_mate, fwd_mate), (mate, sum_mate))[which]
        return pltpu.make_async_remote_copy(
            src_ref=block(i, owner),
            dst_ref=at_rows(dst, i),
            send_sem=mate_send_sem.at[which, i],
            recv_sem=mate_recv_sem.at[which, i],
            device_id={"tp": mate},
            device_id_type=MESH,
        )

    def far_copy(i):
        return pltpu.make_async_remote_copy(
            src_ref=at_rows(fwd_send, i),
            dst_ref=at_rows(sum_far, i),
            send_sem=far_send_sem.at[i],
            recv_sem=far_recv_sem.at[i],
            device_id={"tp": far},
            device_id_type=MESH,
        )

    def hid_copy(k):
        q = lax.rem(p + k, ngroup)
        return pltpu.make_async_remote_copy(
            src_ref=hidden_ref.at[:, :, pl.ds(pl.multiple_of(q * rows, 128), rows)],
            dst_ref=hidden_in_v.at[k - 1],
            send_sem=hid_send_sem.at[k - 1],
            recv_sem=hid_recv_sem.at[k - 1],
            device_id=group_id(k),
            device_id_type=MESH,
        )

    def sq_copy(k):
        return pltpu.make_async_remote_copy(
            src_ref=squares_send,
            dst_ref=squares_all.at[k],
            send_sem=sq_send_sem.at[k],
            recv_sem=sq_recv_sem.at[k],
            device_id=flat_id(k),
            device_id_type=MESH,
        )

    def proj_copy(k):
        return pltpu.make_async_remote_copy(
            src_ref=proj_send.at[pl.ds(k * tokens, tokens)],
            dst_ref=proj_recv.at[k - 1],
            send_sem=proj_send_sem.at[k - 1],
            recv_sem=proj_recv_sem.at[k - 1],
            device_id=group_id(ngroup - k),
            device_id_type=MESH,
        )

    def each(count, fn, start=0):
        def step(i, carry):
            fn(i)
            return carry

        lax.fori_loop(start, count, step, 0)

    each(nchunk, lambda i: local_copy(0, i).start())

    pl.semaphore_wait(barrier, ndev - 1)

    each(nchunk, lambda i: mate_copy(0, i).start())
    each(nchunk, lambda i: mate_copy(1, i).start())
    for k in range(1, ngroup):
        hid_copy(k).start()
    keys_copies = [pltpu.make_async_copy(keys_ref.at[i], keys_v.at[i], cache_sem.at[0, i]) for i in range(nrow)]
    values_copies = [pltpu.make_async_copy(values_ref.at[i], values_v.at[i], cache_sem.at[1, i]) for i in range(nrow)]
    for i in range(nrow):
        keys_copies[i].start()
        values_copies[i].start()
    each(nchunk, lambda i: local_copy(1, i).start())
    loads = [
        pltpu.make_async_copy(src, dst, load_sem.at[i])
        for i, (src, dst) in enumerate(((master_ref, master_v), (one_ref, one_v), (two_ref, two_v)))
    ]
    for copy in loads:
        copy.start()

    query_f[...] = jnp.zeros_like(query_f)
    for i in range(nrow):
        row_q = queries_ref[i].astype(jnp.float32)
        for a in range(heads):
            for j in range(groups):
                n = a * groups + j
                query_f[a, i * PAD + j * nstep : i * PAD + (j + 1) * nstep, :] = row_q[:, n * HD : (n + 1) * HD]

    def forward(i):
        local_copy(0, i).wait()
        mate_copy(0, i).wait_recv()
        at_rows(fwd_send, i)[...] = (at_rows(fwd_own, i)[...] + at_rows(fwd_mate, i)[...]).astype(jnp.bfloat16)
        far_copy(i).start()

    each(nchunk, forward)

    slot = lax.broadcasted_iota(jnp.int32, (PAD, slots), 1)
    for i in range(nrow):
        keys_copies[i].wait()
        values_copies[i].wait()
        valid = slot < lengths_ref[i]
        for a in range(heads):
            q = query_f[a, i * PAD : (i + 1) * PAD, :].astype(jnp.bfloat16)
            scores = lax.dot_general(
                q,
                keys_v[i, :, a * HD : (a + 1) * HD],
                (((1,), (1,)), ((), ())),
                preferred_element_type=jnp.float32,
            )
            scores = jnp.where(valid, scores * scaling, NEG_FILL)
            top = jnp.max(scores, -1, keepdims=True)
            e = jnp.exp(scores - top)
            here = slice(i * PAD, (i + 1) * PAD)
            old_max[a, here, :] = jnp.broadcast_to(top, (PAD, HD))
            old_sum[a, here, :] = jnp.broadcast_to(jnp.sum(e, -1, keepdims=True), (PAD, HD))
            old_out[a, here, :] = jnp.dot(
                e.astype(jnp.bfloat16), values_v[i, :, a * HD : (a + 1) * HD], preferred_element_type=jnp.float32
            )

    for k in range(ngroup):
        if k == 0:
            own = hidden_ref[:, :, pl.ds(pl.multiple_of(p * rows, 128), rows)]
        else:
            hid_copy(k).wait_recv()
            own = hidden_in_v[k - 1]
        for i in range(nrow):
            at = k * tokens + i * nstep
            hidden_f[at : at + nstep, :] = own[i].astype(jnp.float32)

    def total(i, acc):
        local_copy(1, i).wait()
        mate_copy(1, i).wait_recv()
        far_copy(i).wait_recv()
        s = at_rows(sum_own, i)[...] + at_rows(sum_mate, i)[...] + at_rows(sum_far, i)[...].astype(jnp.float32)
        at_rows(grad_total, i)[...] = s
        return acc + jnp.sum((s * s).reshape(CHUNK // 8, 8, cols), axis=0)

    acc = lax.fori_loop(0, nchunk, total, jnp.zeros((8, cols), jnp.float32))
    part = jnp.sum(acc, axis=0, keepdims=True)
    mine = sum(part[:, j * 128 : (j + 1) * 128] for j in range(cols // 128))
    squares_send[...] = mine
    each(ndev, lambda k: sq_copy(k).start(), 1)
    squares_all[0] = mine
    for copy in loads:
        copy.wait()
    each(ndev, lambda k: sq_copy(k).wait_recv(), 1)
    squares = jnp.sum(jnp.sum(squares_all[...], axis=0), axis=1, keepdims=True)
    norm_limit = math.sqrt(D * 2 * KVH * HD)
    factor = jnp.minimum(1.0, norm_limit / jnp.sqrt(jnp.broadcast_to(squares, (1, cols))))

    def adam(i):
        clipped = at_rows(grad_total, i)[...] * factor
        one = BETA_ONE * at_rows(one_v, i)[...] + (1.0 - BETA_ONE) * clipped
        two = BETA_TWO * at_rows(two_v, i)[...] + (1.0 - BETA_TWO) * clipped * clipped
        at_rows(one_v, i)[...] = one
        at_rows(two_v, i)[...] = two
        update = (one * (LEARN_RATE / FIRST_CORR)) / (jnp.sqrt(two * (1.0 / SECOND_CORR)) + EPSILON)
        at_rows(weights_v, i)[...] = (at_rows(master_v, i)[...] - update).astype(jnp.bfloat16)

    each(nchunk, adam)
    proj_send[...] = jnp.dot(hidden_f[...].astype(jnp.bfloat16), weights_v[...], preferred_element_type=jnp.float32)
    for k in range(1, ngroup):
        proj_copy(k).start()
    outs = [
        pltpu.make_async_copy(one_v, one_out, out_sem.at[0]),
        pltpu.make_async_copy(two_v, two_out, out_sem.at[1]),
    ]
    for copy in outs:
        copy.start()

    each(nchunk, lambda i: mate_copy(0, i).wait_send())
    each(nchunk, lambda i: mate_copy(1, i).wait_send())
    each(nchunk, lambda i: far_copy(i).wait_send())
    each(ndev, lambda k: sq_copy(k).wait_send(), 1)
    for k in range(1, ngroup):
        hid_copy(k).wait_send()

    projected = proj_send[0:tokens, :]
    for k in range(1, ngroup):
        proj_copy(k).wait_recv()
        projected = projected + proj_recv[k - 1]

    qi = lax.broadcasted_iota(jnp.int32, (nrow * PAD, tokens), 0)
    kj = lax.broadcasted_iota(jnp.int32, (nrow * PAD, tokens), 1)
    seen = (qi // PAD == kj // nstep) & (qi % nstep >= kj % nstep)
    for a in range(heads):
        k = projected[:, 2 * a * HD : (2 * a + 1) * HD]
        new_k = (k * cos_ref[...] + pltpu.roll(k, HD // 2, 1) * sin_ref[...]).astype(jnp.bfloat16)
        new_v = projected[:, (2 * a + 1) * HD : (2 * a + 2) * HD].astype(jnp.bfloat16)
        entries_out[:, 2 * a * HD : (2 * a + 1) * HD] = new_k.astype(jnp.float32)
        entries_out[:, (2 * a + 1) * HD : (2 * a + 2) * HD] = new_v.astype(jnp.float32)
        scores = lax.dot_general(
            query_f[a].astype(jnp.bfloat16), new_k, (((1,), (1,)), ((), ())), preferred_element_type=jnp.float32
        )
        scores = jnp.where(seen, scores * scaling, NEG_FILL)
        before = old_max[a][:, 0:1]
        top = jnp.maximum(before, jnp.max(scores, -1, keepdims=True))
        alpha = jnp.exp(before - top)
        e = jnp.exp(scores - top)
        whole = old_sum[a][:, 0:1] * alpha + jnp.sum(e, -1, keepdims=True)
        o = old_out[a] * alpha + jnp.dot(e.astype(jnp.bfloat16), new_v, preferred_element_type=jnp.float32)
        old_out[a] = o / whole
        for i in range(nrow):
            for j in range(groups):
                n = a * groups + j
                at = i * PAD + j * nstep
                attended_out[i, :, n * HD : (n + 1) * HD] = old_out[a, at : at + nstep, :]

    for k in range(1, ngroup):
        proj_copy(k).wait_send()
    for copy in outs:
        copy.wait()


def fused_body(
    sizes,
    grad_parts,
    master,
    moment_one,
    moment_two,
    hidden_in,
    queries,
    cache_keys,
    cache_values,
    cache_lengths,
):
    ngrp, nrep, ntp = sizes
    ngroup = ngrp * nrep
    ndev = ngroup * ntp
    rows, cols = master.shape
    nrow, nstep, width = hidden_in.shape
    tokens = nrow * nstep
    slots = cache_keys.shape[1]
    heads = cols // (2 * HD)
    nchunk = rows // CHUNK
    half = HD // 2
    inverse = jnp.exp(-math.log(ROPE_BASE) * 2.0 * jnp.arange(half, dtype=jnp.float32) / HD)
    positions = (cache_lengths[:, None] + jnp.arange(nstep, dtype=jnp.int32)[None, :]).astype(jnp.float32)
    angles = positions.reshape(tokens, 1) * inverse[None, :]
    cos = jnp.concatenate([jnp.cos(angles)] * 2, -1)
    sin = jnp.concatenate([-jnp.sin(angles), jnp.sin(angles)], -1)
    f32, bf16 = jnp.float32, jnp.bfloat16
    vm = pltpu.VMEM
    dma = pltpu.SemaphoreType.DMA
    vmem = pl.BlockSpec(memory_space=pltpu.VMEM)
    hbm = pl.BlockSpec(memory_space=pltpu.HBM)
    smem = pl.BlockSpec(memory_space=pltpu.SMEM)
    new_one, new_two, entries, attended = pl.pallas_call(
        functools.partial(fused_kernel, sizes),
        out_shape=(
            jax.ShapeDtypeStruct((rows, cols), f32),
            jax.ShapeDtypeStruct((rows, cols), f32),
            jax.ShapeDtypeStruct((tokens, cols), f32),
            jax.ShapeDtypeStruct(queries.shape, f32),
        ),
        in_specs=[smem, vmem, vmem, vmem, vmem] + [hbm] * 6,
        out_specs=(hbm, hbm, vmem, vmem),
        scratch_shapes=[
            vm((rows, cols), f32),
            vm((rows, cols), f32),
            vm((rows, cols), f32),
            vm((rows, cols), f32),
            vm((rows, cols), bf16),
            vm((rows, cols), bf16),
            vm((rows, cols), f32),
            vm((rows, cols), f32),
            vm((rows, cols), f32),
            vm((rows, cols), f32),
            vm(cache_keys.shape, bf16),
            vm(cache_values.shape, bf16),
            vm((ngroup - 1, nrow, nstep, rows), bf16),
            vm((ngroup * tokens, rows), f32),
            vm((rows, cols), bf16),
            vm((1, 128), f32),
            vm((ndev, 1, 128), f32),
            vm((ngroup * tokens, cols), f32),
            vm((ngroup - 1, tokens, cols), f32),
            vm((heads, nrow * PAD, HD), f32),
            vm((heads, nrow * PAD, HD), f32),
            vm((heads, nrow * PAD, HD), f32),
            vm((heads, nrow * PAD, HD), f32),
            dma((2, nchunk)),
            dma((2, nchunk)),
            dma((2, nchunk)),
            dma((nchunk,)),
            dma((nchunk,)),
            dma((ngroup - 1,)),
            dma((ngroup - 1,)),
            dma((ndev,)),
            dma((ndev,)),
            dma((ngroup - 1,)),
            dma((ngroup - 1,)),
            dma((3,)),
            dma((2, nrow)),
            dma((2,)),
        ],
        compiler_params=pltpu.CompilerParams(
            collective_id=0, has_side_effects=True, vmem_limit_bytes=48 * 1024 * 1024
        ),
    )(
        cache_lengths, cos, sin, hidden_in, queries, grad_parts, master, moment_one, moment_two, cache_keys, cache_values
    )
    return (
        new_one,
        new_two,
        entries.astype(bf16).reshape(nrow, nstep, cols),
        attended.astype(bf16),
    )


def solution(mesh):
    sizes = (mesh.shape["grp"], mesh.shape["rep"], mesh.shape["tp"])
    fits = sizes[2] == 4 and D % (sizes[0] * sizes[1] * 128) == 0 and (KVH % sizes[2]) == 0
    placed = (
        P("tp", ("grp", "rep"), None),
        P(("grp", "rep"), "tp"),
        P(("grp", "rep"), "tp"),
        P(("grp", "rep"), "tp"),
        P(("grp", "rep"), None, None),
        P(("grp", "rep"), None, "tp"),
        P(("grp", "rep"), None, "tp"),
        P(("grp", "rep"), None, "tp"),
        P(("grp", "rep")),
    )
    return jax.shard_map(
        functools.partial(fused_body, sizes) if fits else body,
        mesh=mesh,
        in_specs=placed,
        out_specs=(
            P(("grp", "rep"), "tp"),
            P(("grp", "rep"), "tp"),
            P(("grp", "rep"), None, "tp"),
            P(("grp", "rep"), None, "tp"),
        ),
        check_vma=False,
    )
```

```python
import functools
import math

import jax
import jax.numpy as jnp
from jax import lax
from jax.experimental import pallas as pl
from jax.experimental.pallas import tpu as pltpu
from jax.sharding import PartitionSpec as P

D = 5120
QH = 40
KVH = 8
HD = 128


BETA_ONE = 0.9
BETA_TWO = 0.999
FIRST_CORR = 0.9999734386011124
SECOND_CORR = 0.09520785288629041
LEARN_RATE = 0.003
EPSILON = 1e-08
ROPE_BASE = 1000000.0
NEG_FILL = -1e30


def rotate(new_keys, lengths):
    positions = (lengths[:, None] + jnp.arange(new_keys.shape[1], dtype=jnp.int32)[None, :]).astype(
        jnp.float32
    )
    half_dim = new_keys.shape[-1] // 2
    inverse = jnp.exp(
        -math.log(ROPE_BASE) * 2.0 * jnp.arange(half_dim, dtype=jnp.float32) / new_keys.shape[-1]
    )
    angles = positions[:, :, None] * inverse[None, None, :]
    cosine_part = jnp.concatenate([jnp.cos(angles), jnp.cos(angles)], -1)[:, :, None, :]
    sine_part = jnp.concatenate([jnp.sin(angles), jnp.sin(angles)], -1)[:, :, None, :]
    rotated = jnp.concatenate([-new_keys[..., half_dim:], new_keys[..., :half_dim]], -1)
    return new_keys * cosine_part + rotated * sine_part


def body(
    grad_parts,
    master,
    moment_one,
    moment_two,
    hidden_in,
    queries,
    cache_keys,
    cache_values,
    cache_lengths,
):
    col_width = master.shape[1]
    grad_sum = lax.psum_scatter(grad_parts[0], "tp", scatter_dimension=1, tiled=True)
    squares = lax.psum(jnp.sum(grad_sum * grad_sum), ("grp", "rep", "tp"))
    norm_limit = math.sqrt(D * 2 * KVH * HD)
    clipped = grad_sum * jnp.minimum(1.0, norm_limit / jnp.sqrt(squares))
    new_moment_one = BETA_ONE * moment_one + (1.0 - BETA_ONE) * clipped
    new_moment_two = BETA_TWO * moment_two + (1.0 - BETA_TWO) * clipped * clipped
    update = new_moment_one / FIRST_CORR / (jnp.sqrt(new_moment_two / SECOND_CORR) + EPSILON)
    weights = (master - LEARN_RATE * update).astype(jnp.bfloat16)
    row_count, step_count, model_width = hidden_in.shape
    token_count = row_count * step_count
    flat_inputs = hidden_in.reshape(token_count, model_width)
    sliced = lax.all_to_all(
        lax.all_to_all(flat_inputs, "grp", split_axis=1, concat_axis=0, tiled=True),
        "rep",
        split_axis=1,
        concat_axis=0,
        tiled=True,
    )
    group_count = lax.axis_size("grp")
    replica_count = lax.axis_size("rep")
    ordered = sliced.reshape(replica_count, group_count, token_count, weights.shape[0])
    ordered = jnp.swapaxes(ordered, 0, 1).reshape(
        group_count * replica_count * token_count, weights.shape[0]
    )
    projected = lax.psum_scatter(
        jnp.dot(ordered, weights, preferred_element_type=jnp.float32),
        ("grp", "rep"),
        scatter_dimension=0,
        tiled=True,
    )
    heads_here = col_width // (2 * HD)
    projected = projected.reshape(row_count, step_count, heads_here, 2, HD)
    new_keys = rotate(projected[:, :, :, 0, :], cache_lengths).astype(jnp.bfloat16)
    new_values = projected[:, :, :, 1, :].astype(jnp.bfloat16)
    new_entries = jnp.stack([new_keys, new_values], 3).reshape(row_count, step_count, col_width)
    groups = QH // KVH
    slots = cache_keys.shape[1]
    query_heads = queries.reshape(row_count, step_count, heads_here, groups, HD)
    old_k = cache_keys.reshape(row_count, slots, heads_here, HD)
    old_v = cache_values.reshape(row_count, slots, heads_here, HD)
    scaling = 1.0 / math.sqrt(HD)
    old_scores = (
        jnp.einsum("rsagd,rjad->rsagj", query_heads, old_k, preferred_element_type=jnp.float32)
        * scaling
    )
    valid_slots = jnp.arange(slots, dtype=jnp.int32)[None, :] < cache_lengths[:, None]
    old_scores = jnp.where(valid_slots[:, None, None, None, :], old_scores, NEG_FILL)
    new_scores = (
        jnp.einsum("rsagd,rtad->rsagt", query_heads, new_keys, preferred_element_type=jnp.float32)
        * scaling
    )
    causal = jnp.arange(step_count)[:, None] >= jnp.arange(step_count)[None, :]
    new_scores = jnp.where(causal[None, :, None, None, :], new_scores, NEG_FILL)
    scores = jnp.concatenate([old_scores, new_scores], -1)
    row_max = jnp.max(scores, -1, keepdims=True)
    exp_scores = jnp.exp(scores - row_max)
    probs = (exp_scores / jnp.sum(exp_scores, -1, keepdims=True)).astype(jnp.bfloat16)
    output = jnp.einsum(
        "rsagj,rjad->rsagd", probs[..., :slots], old_v, preferred_element_type=jnp.float32
    )
    output = output + jnp.einsum(
        "rsagt,rtad->rsagd", probs[..., slots:], new_values, preferred_element_type=jnp.float32
    )
    attended = output.reshape(row_count, step_count, heads_here * groups * HD).astype(jnp.bfloat16)
    return (new_moment_one, new_moment_two, new_entries, attended)


MESH = pl.DeviceIdType.MESH
CHUNK = 64
PAD = 32


def fused_kernel(
    sizes,
    lengths_ref,
    hidden_ref,
    queries_ref,
    grad_ref,
    master_ref,
    one_ref,
    two_ref,
    keys_ref,
    values_ref,
    one_out,
    two_out,
    proj_out,
    cos_out,
    sin_out,
    query_f,
    old_max,
    old_sum,
    old_out,
    lengths_s,
    queries_v,
    fwd_own,
    fwd_mate,
    sum_own,
    sum_mate,
    fwd_send,
    sum_far,
    grad_total,
    master_v,
    one_v,
    two_v,
    keys_v,
    values_v,
    hidden_in_v,
    hidden_f,
    weights_v,
    squares_send,
    squares_all,
    proj_own,
    proj_send,
    proj_recv,
    local_sem,
    mate_send_sem,
    mate_recv_sem,
    far_send_sem,
    far_recv_sem,
    hid_send_sem,
    hid_recv_sem,
    sq_send_sem,
    sq_recv_sem,
    proj_send_sem,
    proj_recv_sem,
    load_sem,
    cache_sem,
    small_sem,
):
    ngrp, nrep, ntp = sizes
    ngroup = ngrp * nrep
    ndev = ngroup * ntp
    rows, cols = master_ref.shape
    nrow, nstep, width = hidden_ref.shape
    tokens = nrow * nstep
    slots = keys_ref.shape[1]
    heads = cols // (2 * HD)
    groups = QH // KVH
    nchunk = rows // CHUNK
    scaling = 1.0 / math.sqrt(HD)

    g = lax.axis_index("grp")
    r = lax.axis_index("rep")
    t = lax.axis_index("tp")
    p = g * nrep + r
    flat = p * ntp + t
    y = t // 2
    c = t % 2
    mate = y * 2 + (1 - c)
    far = (1 - y) * 2 + c
    far_mate = (1 - y) * 2 + (1 - c)

    def flat_id(k):
        f = lax.rem(flat + k, ndev)
        q = f // ntp
        return {"grp": q // nrep, "rep": lax.rem(q, nrep), "tp": lax.rem(f, ntp)}

    def group_id(k):
        q = lax.rem(p + k, ngroup)
        return {"grp": q // nrep, "rep": lax.rem(q, nrep)}

    barrier = pltpu.get_barrier_semaphore()

    def greet(k, carry):
        pl.semaphore_signal(barrier, inc=1, device_id=flat_id(k), device_id_type=MESH)
        return carry

    lax.fori_loop(1, ndev, greet, 0)

    def block(i, owner):
        return grad_ref.at[0, pl.ds(pl.multiple_of(i * CHUNK, CHUNK), CHUNK), pl.ds(pl.multiple_of(owner * cols, cols), cols)]

    def at_rows(ref, i):
        return ref.at[pl.ds(pl.multiple_of(i * CHUNK, CHUNK), CHUNK)]

    def local_copy(which, i):
        owner, dst = ((far, fwd_own), (t, sum_own))[which]
        return pltpu.make_async_copy(block(i, owner), at_rows(dst, i), local_sem.at[which, i])

    def mate_copy(which, i):
        owner, dst = ((far_mate, fwd_mate), (mate, sum_mate))[which]
        return pltpu.make_async_remote_copy(
            src_ref=block(i, owner),
            dst_ref=at_rows(dst, i),
            send_sem=mate_send_sem.at[which, i],
            recv_sem=mate_recv_sem.at[which, i],
            device_id={"tp": mate},
            device_id_type=MESH,
        )

    def far_copy(i):
        return pltpu.make_async_remote_copy(
            src_ref=at_rows(fwd_send, i),
            dst_ref=at_rows(sum_far, i),
            send_sem=far_send_sem.at[i],
            recv_sem=far_recv_sem.at[i],
            device_id={"tp": far},
            device_id_type=MESH,
        )

    def hid_copy(k):
        q = lax.rem(p + k, ngroup)
        return pltpu.make_async_remote_copy(
            src_ref=hidden_ref.at[:, :, pl.ds(pl.multiple_of(q * rows, 128), rows)],
            dst_ref=hidden_in_v.at[k],
            send_sem=hid_send_sem.at[k - 1],
            recv_sem=hid_recv_sem.at[k - 1],
            device_id=group_id(k),
            device_id_type=MESH,
        )

    def sq_copy(k):
        return pltpu.make_async_remote_copy(
            src_ref=squares_send,
            dst_ref=squares_all.at[k],
            send_sem=sq_send_sem.at[k],
            recv_sem=sq_recv_sem.at[k],
            device_id=flat_id(k),
            device_id_type=MESH,
        )

    def proj_copy(k):
        return pltpu.make_async_remote_copy(
            src_ref=proj_send.at[k - 1],
            dst_ref=proj_recv.at[k - 1],
            send_sem=proj_send_sem.at[k - 1],
            recv_sem=proj_recv_sem.at[k - 1],
            device_id=group_id(ngroup - k),
            device_id_type=MESH,
        )

    def each(count, fn, start=0):
        def step(i, carry):
            fn(i)
            return carry

        lax.fori_loop(start, count, step, 0)

    each(nchunk, lambda i: local_copy(0, i).start())
    small = [
        pltpu.make_async_copy(src, dst, small_sem.at[i])
        for i, (src, dst) in enumerate(
            (
                (lengths_ref, lengths_s),
                (queries_ref, queries_v),
                (hidden_ref.at[:, :, pl.ds(pl.multiple_of(p * rows, 128), rows)], hidden_in_v.at[0]),
            )
        )
    ]
    for copy in small:
        copy.start()

    pl.semaphore_wait(barrier, ndev - 1)

    each(nchunk, lambda i: mate_copy(0, i).start())
    each(nchunk, lambda i: mate_copy(1, i).start())
    for k in range(1, ngroup):
        hid_copy(k).start()
    keys_copies = [pltpu.make_async_copy(keys_ref.at[i], keys_v.at[i], cache_sem.at[0, i]) for i in range(nrow)]
    values_copies = [pltpu.make_async_copy(values_ref.at[i], values_v.at[i], cache_sem.at[1, i]) for i in range(nrow)]
    for i in range(nrow):
        keys_copies[i].start()
        values_copies[i].start()
    each(nchunk, lambda i: local_copy(1, i).start())
    loads = [
        pltpu.make_async_copy(src, dst, load_sem.at[i])
        for i, (src, dst) in enumerate(((master_ref, master_v), (one_ref, one_v), (two_ref, two_v)))
    ]
    for copy in loads:
        copy.start()

    for copy in small:
        copy.wait()
    query_f[...] = jnp.zeros_like(query_f)
    for i in range(nrow):
        row_q = queries_v[i].astype(jnp.float32)
        for a in range(heads):
            for j in range(groups):
                n = a * groups + j
                query_f[a, i * PAD + j * nstep : i * PAD + (j + 1) * nstep, :] = row_q[:, n * HD : (n + 1) * HD]

    def forward(i):
        local_copy(0, i).wait()
        mate_copy(0, i).wait_recv()
        at_rows(fwd_send, i)[...] = (at_rows(fwd_own, i)[...] + at_rows(fwd_mate, i)[...]).astype(jnp.bfloat16)
        far_copy(i).start()

    each(nchunk, forward)

    slot = lax.broadcasted_iota(jnp.int32, (PAD, slots), 1)
    for i in range(nrow):
        keys_copies[i].wait()
        values_copies[i].wait()
        valid = slot < lengths_s[i]
        for a in range(heads):
            q = query_f[a, i * PAD : (i + 1) * PAD, :].astype(jnp.bfloat16)
            scores = lax.dot_general(
                q,
                keys_v[i, :, a * HD : (a + 1) * HD],
                (((1,), (1,)), ((), ())),
                preferred_element_type=jnp.float32,
            )
            scores = jnp.where(valid, scores * scaling, NEG_FILL)
            top = jnp.max(scores, -1, keepdims=True)
            e = jnp.exp(scores - top)
            here = slice(i * PAD, (i + 1) * PAD)
            old_max[a, here, :] = jnp.broadcast_to(top, (PAD, HD))
            old_sum[a, here, :] = jnp.broadcast_to(jnp.sum(e, -1, keepdims=True), (PAD, HD))
            old_out[a, here, :] = jnp.dot(
                e.astype(jnp.bfloat16), values_v[i, :, a * HD : (a + 1) * HD], preferred_element_type=jnp.float32
            )

    for k in range(ngroup):
        if k > 0:
            hid_copy(k).wait_recv()
        own = hidden_in_v[k]
        for i in range(nrow):
            at = k * tokens + i * nstep
            hidden_f[at : at + nstep, :] = own[i].astype(jnp.float32)

    token = lax.broadcasted_iota(jnp.int32, (tokens, HD), 0)
    lane = lax.broadcasted_iota(jnp.int32, (tokens, HD), 1)
    position = lax.rem(token, nstep)
    for i in range(nrow):
        position = position + jnp.where(token // nstep == i, lengths_s[i], 0)
    pair = lax.rem(lane, HD // 2).astype(jnp.float32)
    angle = position.astype(jnp.float32) * jnp.exp(-math.log(ROPE_BASE) * 2.0 * pair / HD)
    cos_out[...] = jnp.cos(angle)
    sin_out[...] = jnp.where(lane < HD // 2, -jnp.sin(angle), jnp.sin(angle))

    def total(i, acc):
        local_copy(1, i).wait()
        mate_copy(1, i).wait_recv()
        far_copy(i).wait_recv()
        s = at_rows(sum_own, i)[...] + at_rows(sum_mate, i)[...] + at_rows(sum_far, i)[...].astype(jnp.float32)
        at_rows(grad_total, i)[...] = s
        return acc + jnp.sum((s * s).reshape(CHUNK // 8, 8, cols), axis=0)

    acc = lax.fori_loop(0, nchunk, total, jnp.zeros((8, cols), jnp.float32))
    part = jnp.sum(acc, axis=0, keepdims=True)
    mine = sum(part[:, j * 128 : (j + 1) * 128] for j in range(cols // 128))
    squares_send[...] = mine
    each(ndev, lambda k: sq_copy(k).start(), 1)
    squares_all[0] = mine
    for copy in loads:
        copy.wait()
    each(ndev, lambda k: sq_copy(k).wait_recv(), 1)
    squares = jnp.sum(jnp.sum(squares_all[...], axis=0), axis=1, keepdims=True)
    norm_limit = math.sqrt(D * 2 * KVH * HD)
    factor = jnp.minimum(1.0, norm_limit / jnp.sqrt(jnp.broadcast_to(squares, (1, cols))))

    def adam(i):
        clipped = at_rows(grad_total, i)[...] * factor
        one = BETA_ONE * at_rows(one_v, i)[...] + (1.0 - BETA_ONE) * clipped
        two = BETA_TWO * at_rows(two_v, i)[...] + (1.0 - BETA_TWO) * clipped * clipped
        at_rows(one_out, i)[...] = one
        at_rows(two_out, i)[...] = two
        update = (one * (LEARN_RATE / FIRST_CORR)) / (jnp.sqrt(two * (1.0 / SECOND_CORR)) + EPSILON)
        at_rows(weights_v, i)[...] = (at_rows(master_v, i)[...] - update).astype(jnp.bfloat16)

    each(nchunk, adam)
    partial = jnp.dot(hidden_f[...].astype(jnp.bfloat16), weights_v[...], preferred_element_type=jnp.float32)
    for k in range(1, ngroup):
        proj_send[k - 1] = partial[k * tokens : (k + 1) * tokens].astype(jnp.bfloat16)
        proj_copy(k).start()
    proj_own[...] = partial[0:tokens]

    each(nchunk, lambda i: mate_copy(0, i).wait_send())
    each(nchunk, lambda i: mate_copy(1, i).wait_send())
    each(nchunk, lambda i: far_copy(i).wait_send())
    each(ndev, lambda k: sq_copy(k).wait_send(), 1)
    for k in range(1, ngroup):
        hid_copy(k).wait_send()

    projected = proj_own[...]
    for k in range(1, ngroup):
        proj_copy(k).wait_recv()
        projected = projected + proj_recv[k - 1].astype(jnp.float32)
    proj_out[...] = projected
    for k in range(1, ngroup):
        proj_copy(k).wait_send()


def finish_kernel(
    one_ref,
    two_ref,
    proj_ref,
    cos_ref,
    sin_ref,
    query_ref,
    max_ref,
    sum_ref,
    old_ref,
    one_out,
    two_out,
    entries_out,
    attended_out,
    heads_v,
    out_sem,
):
    outs = [
        pltpu.make_async_copy(one_ref, one_out, out_sem.at[0]),
        pltpu.make_async_copy(two_ref, two_out, out_sem.at[1]),
    ]
    for copy in outs:
        copy.start()
    nrow, nstep, cols = entries_out.shape
    tokens = nrow * nstep
    heads = cols // (2 * HD)
    groups = QH // KVH
    scaling = 1.0 / math.sqrt(HD)
    qi = lax.broadcasted_iota(jnp.int32, (nrow * PAD, tokens), 0)
    kj = lax.broadcasted_iota(jnp.int32, (nrow * PAD, tokens), 1)
    seen = (qi // PAD == kj // nstep) & (qi % nstep >= kj % nstep)
    for a in range(heads):
        k = proj_ref[:, 2 * a * HD : (2 * a + 1) * HD]
        k = k * cos_ref[...] + pltpu.roll(k, HD // 2, 1) * sin_ref[...]
        v = proj_ref[:, (2 * a + 1) * HD : (2 * a + 2) * HD]
        new_k = k.astype(jnp.bfloat16)
        new_v = v.astype(jnp.bfloat16)
        for i in range(nrow):
            rows_i = slice(i * nstep, (i + 1) * nstep)
            entries_out[i, :, 2 * a * HD : (2 * a + 1) * HD] = k[rows_i].astype(jnp.bfloat16)
            entries_out[i, :, (2 * a + 1) * HD : (2 * a + 2) * HD] = v[rows_i].astype(jnp.bfloat16)
        scores = lax.dot_general(
            query_ref[a].astype(jnp.bfloat16), new_k, (((1,), (1,)), ((), ())), preferred_element_type=jnp.float32
        )
        scores = jnp.where(seen, scores * scaling, NEG_FILL)
        before = max_ref[a][:, 0:1]
        top = jnp.maximum(before, jnp.max(scores, -1, keepdims=True))
        alpha = jnp.exp(before - top)
        e = jnp.exp(scores - top)
        whole = sum_ref[a][:, 0:1] * alpha + jnp.sum(e, -1, keepdims=True)
        o = old_ref[a] * alpha + jnp.dot(e.astype(jnp.bfloat16), new_v, preferred_element_type=jnp.float32)
        heads_v[a] = o / whole
        for i in range(nrow):
            for j in range(groups):
                n = a * groups + j
                at = i * PAD + j * nstep
                attended_out[i, :, n * HD : (n + 1) * HD] = heads_v[a, at : at + nstep, :].astype(jnp.bfloat16)
    for copy in outs:
        copy.wait()


def fused_body(
    sizes,
    grad_parts,
    master,
    moment_one,
    moment_two,
    hidden_in,
    queries,
    cache_keys,
    cache_values,
    cache_lengths,
):
    ngrp, nrep, ntp = sizes
    ngroup = ngrp * nrep
    ndev = ngroup * ntp
    rows, cols = master.shape
    nrow, nstep, width = hidden_in.shape
    tokens = nrow * nstep
    heads = cols // (2 * HD)
    nchunk = rows // CHUNK
    f32, bf16 = jnp.float32, jnp.bfloat16
    vm = pltpu.VMEM
    dma = pltpu.SemaphoreType.DMA
    vmem = pl.BlockSpec(memory_space=pltpu.VMEM)
    hbm = pl.BlockSpec(memory_space=pltpu.HBM)
    per_head = vm((heads, nrow * PAD, HD), f32)
    moment = vm((rows, cols), f32)
    table = vm((tokens, HD), f32)
    middle = pl.pallas_call(
        functools.partial(fused_kernel, sizes),
        out_shape=(moment, moment, vm((tokens, cols), f32), table, table) + (per_head,) * 4,
        in_specs=[hbm] * 9,
        out_specs=(vmem,) * 9,
        scratch_shapes=[
            pltpu.SMEM((nrow,), jnp.int32),
            vm(queries.shape, bf16),
            vm((rows, cols), f32),
            vm((rows, cols), f32),
            vm((rows, cols), f32),
            vm((rows, cols), f32),
            vm((rows, cols), bf16),
            vm((rows, cols), bf16),
            vm((rows, cols), f32),
            vm((rows, cols), f32),
            vm((rows, cols), f32),
            vm((rows, cols), f32),
            vm(cache_keys.shape, bf16),
            vm(cache_values.shape, bf16),
            vm((ngroup, nrow, nstep, rows), bf16),
            vm((ngroup * tokens, rows), f32),
            vm((rows, cols), bf16),
            vm((1, 128), f32),
            vm((ndev, 1, 128), f32),
            vm((tokens, cols), f32),
            vm((ngroup - 1, tokens, cols), bf16),
            vm((ngroup - 1, tokens, cols), bf16),
            dma((2, nchunk)),
            dma((2, nchunk)),
            dma((2, nchunk)),
            dma((nchunk,)),
            dma((nchunk,)),
            dma((ngroup - 1,)),
            dma((ngroup - 1,)),
            dma((ndev,)),
            dma((ndev,)),
            dma((ngroup - 1,)),
            dma((ngroup - 1,)),
            dma((3,)),
            dma((2, nrow)),
            dma((3,)),
        ],
        compiler_params=pltpu.CompilerParams(
            collective_id=0, has_side_effects=True, vmem_limit_bytes=60 * 1024 * 1024 + 320 * 1024
        ),
    )(cache_lengths, hidden_in, queries, grad_parts, master, moment_one, moment_two, cache_keys, cache_values)
    return pl.pallas_call(
        finish_kernel,
        out_shape=(
            jax.ShapeDtypeStruct((rows, cols), f32),
            jax.ShapeDtypeStruct((rows, cols), f32),
            jax.ShapeDtypeStruct((nrow, nstep, cols), bf16),
            jax.ShapeDtypeStruct(queries.shape, bf16),
        ),
        in_specs=[vmem] * 9,
        out_specs=(hbm, hbm, vmem, vmem),
        scratch_shapes=[vm((heads, nrow * PAD, HD), f32), dma((2,))],
        compiler_params=pltpu.CompilerParams(vmem_limit_bytes=8 * 1024 * 1024),
    )(*middle)


def solution(mesh):
    sizes = (mesh.shape["grp"], mesh.shape["rep"], mesh.shape["tp"])
    fits = sizes[2] == 4 and D % (sizes[0] * sizes[1] * 128) == 0 and (KVH % sizes[2]) == 0
    placed = (
        P("tp", ("grp", "rep"), None),
        P(("grp", "rep"), "tp"),
        P(("grp", "rep"), "tp"),
        P(("grp", "rep"), "tp"),
        P(("grp", "rep"), None, None),
        P(("grp", "rep"), None, "tp"),
        P(("grp", "rep"), None, "tp"),
        P(("grp", "rep"), None, "tp"),
        P(("grp", "rep")),
    )
    return jax.shard_map(
        functools.partial(fused_body, sizes) if fits else body,
        mesh=mesh,
        in_specs=placed,
        out_specs=(
            P(("grp", "rep"), "tp"),
            P(("grp", "rep"), "tp"),
            P(("grp", "rep"), None, "tp"),
            P(("grp", "rep"), None, "tp"),
        ),
        check_vma=False,
    )
```

```python
import functools
import math

import jax
import jax.numpy as jnp
from jax import lax
from jax.experimental import pallas as pl
from jax.experimental.pallas import tpu as pltpu
from jax.sharding import PartitionSpec as P

D = 5120
QH = 40
KVH = 8
HD = 128


BETA_ONE = 0.9
BETA_TWO = 0.999
FIRST_CORR = 0.9999734386011124
SECOND_CORR = 0.09520785288629041
LEARN_RATE = 0.003
EPSILON = 1e-08
ROPE_BASE = 1000000.0
NEG_FILL = -1e30


def rotate(new_keys, lengths):
    positions = (lengths[:, None] + jnp.arange(new_keys.shape[1], dtype=jnp.int32)[None, :]).astype(
        jnp.float32
    )
    half_dim = new_keys.shape[-1] // 2
    inverse = jnp.exp(
        -math.log(ROPE_BASE) * 2.0 * jnp.arange(half_dim, dtype=jnp.float32) / new_keys.shape[-1]
    )
    angles = positions[:, :, None] * inverse[None, None, :]
    cosine_part = jnp.concatenate([jnp.cos(angles), jnp.cos(angles)], -1)[:, :, None, :]
    sine_part = jnp.concatenate([jnp.sin(angles), jnp.sin(angles)], -1)[:, :, None, :]
    rotated = jnp.concatenate([-new_keys[..., half_dim:], new_keys[..., :half_dim]], -1)
    return new_keys * cosine_part + rotated * sine_part


def body(
    grad_parts,
    master,
    moment_one,
    moment_two,
    hidden_in,
    queries,
    cache_keys,
    cache_values,
    cache_lengths,
):
    col_width = master.shape[1]
    grad_sum = lax.psum_scatter(grad_parts[0], "tp", scatter_dimension=1, tiled=True)
    squares = lax.psum(jnp.sum(grad_sum * grad_sum), ("grp", "rep", "tp"))
    norm_limit = math.sqrt(D * 2 * KVH * HD)
    clipped = grad_sum * jnp.minimum(1.0, norm_limit / jnp.sqrt(squares))
    new_moment_one = BETA_ONE * moment_one + (1.0 - BETA_ONE) * clipped
    new_moment_two = BETA_TWO * moment_two + (1.0 - BETA_TWO) * clipped * clipped
    update = new_moment_one / FIRST_CORR / (jnp.sqrt(new_moment_two / SECOND_CORR) + EPSILON)
    weights = (master - LEARN_RATE * update).astype(jnp.bfloat16)
    row_count, step_count, model_width = hidden_in.shape
    token_count = row_count * step_count
    flat_inputs = hidden_in.reshape(token_count, model_width)
    sliced = lax.all_to_all(
        lax.all_to_all(flat_inputs, "grp", split_axis=1, concat_axis=0, tiled=True),
        "rep",
        split_axis=1,
        concat_axis=0,
        tiled=True,
    )
    group_count = lax.axis_size("grp")
    replica_count = lax.axis_size("rep")
    ordered = sliced.reshape(replica_count, group_count, token_count, weights.shape[0])
    ordered = jnp.swapaxes(ordered, 0, 1).reshape(
        group_count * replica_count * token_count, weights.shape[0]
    )
    projected = lax.psum_scatter(
        jnp.dot(ordered, weights, preferred_element_type=jnp.float32),
        ("grp", "rep"),
        scatter_dimension=0,
        tiled=True,
    )
    heads_here = col_width // (2 * HD)
    projected = projected.reshape(row_count, step_count, heads_here, 2, HD)
    new_keys = rotate(projected[:, :, :, 0, :], cache_lengths).astype(jnp.bfloat16)
    new_values = projected[:, :, :, 1, :].astype(jnp.bfloat16)
    new_entries = jnp.stack([new_keys, new_values], 3).reshape(row_count, step_count, col_width)
    groups = QH // KVH
    slots = cache_keys.shape[1]
    query_heads = queries.reshape(row_count, step_count, heads_here, groups, HD)
    old_k = cache_keys.reshape(row_count, slots, heads_here, HD)
    old_v = cache_values.reshape(row_count, slots, heads_here, HD)
    scaling = 1.0 / math.sqrt(HD)
    old_scores = (
        jnp.einsum("rsagd,rjad->rsagj", query_heads, old_k, preferred_element_type=jnp.float32)
        * scaling
    )
    valid_slots = jnp.arange(slots, dtype=jnp.int32)[None, :] < cache_lengths[:, None]
    old_scores = jnp.where(valid_slots[:, None, None, None, :], old_scores, NEG_FILL)
    new_scores = (
        jnp.einsum("rsagd,rtad->rsagt", query_heads, new_keys, preferred_element_type=jnp.float32)
        * scaling
    )
    causal = jnp.arange(step_count)[:, None] >= jnp.arange(step_count)[None, :]
    new_scores = jnp.where(causal[None, :, None, None, :], new_scores, NEG_FILL)
    scores = jnp.concatenate([old_scores, new_scores], -1)
    row_max = jnp.max(scores, -1, keepdims=True)
    exp_scores = jnp.exp(scores - row_max)
    probs = (exp_scores / jnp.sum(exp_scores, -1, keepdims=True)).astype(jnp.bfloat16)
    output = jnp.einsum(
        "rsagj,rjad->rsagd", probs[..., :slots], old_v, preferred_element_type=jnp.float32
    )
    output = output + jnp.einsum(
        "rsagt,rtad->rsagd", probs[..., slots:], new_values, preferred_element_type=jnp.float32
    )
    attended = output.reshape(row_count, step_count, heads_here * groups * HD).astype(jnp.bfloat16)
    return (new_moment_one, new_moment_two, new_entries, attended)


MESH = pl.DeviceIdType.MESH
CHUNK = 64
PAD = 32


def fused_kernel(
    sizes,
    lengths_ref,
    hidden_ref,
    queries_ref,
    grad_ref,
    master_ref,
    one_ref,
    two_ref,
    keys_ref,
    values_ref,
    one_out,
    two_out,
    proj_out,
    cos_out,
    sin_out,
    query_f,
    old_max,
    old_sum,
    old_out,
    lengths_s,
    queries_v,
    fwd_own,
    fwd_mate,
    sum_own,
    sum_mate,
    fwd_send,
    sum_far,
    grad_total,
    master_v,
    one_v,
    two_v,
    keys_v,
    values_v,
    hidden_in_v,
    hidden_f,
    weights_v,
    squares_send,
    squares_all,
    proj_own,
    proj_send,
    proj_recv,
    local_sem,
    mate_send_sem,
    mate_recv_sem,
    far_send_sem,
    far_recv_sem,
    hid_send_sem,
    hid_recv_sem,
    sq_send_sem,
    sq_recv_sem,
    proj_send_sem,
    proj_recv_sem,
    load_sem,
    cache_sem,
    small_sem,
    round_sem,
):
    ngrp, nrep, ntp = sizes
    ngroup = ngrp * nrep
    ndev = ngroup * ntp
    rows, cols = master_ref.shape
    nrow, nstep, width = hidden_ref.shape
    tokens = nrow * nstep
    slots = keys_ref.shape[1]
    heads = cols // (2 * HD)
    groups = QH // KVH
    nchunk = rows // CHUNK
    scaling = 1.0 / math.sqrt(HD)

    g = lax.axis_index("grp")
    r = lax.axis_index("rep")
    t = lax.axis_index("tp")
    p = g * nrep + r
    flat = p * ntp + t
    y = t // 2
    c = t % 2
    mate = y * 2 + (1 - c)
    far = (1 - y) * 2 + c
    far_mate = (1 - y) * 2 + (1 - c)

    def flat_id(k):
        f = lax.rem(flat + k, ndev)
        q = f // ntp
        return {"grp": q // nrep, "rep": lax.rem(q, nrep), "tp": lax.rem(f, ntp)}

    def group_id(k):
        q = lax.rem(p + k, ngroup)
        return {"grp": q // nrep, "rep": lax.rem(q, nrep)}

    barrier = pltpu.get_barrier_semaphore()

    bits = ndev.bit_length() - 1

    def across(b):
        stride = 1 << b
        return flat_id(ndev + stride * (1 - 2 * lax.rem(flat // stride, 2)))

    for b in range(bits):
        pl.semaphore_signal(barrier, inc=1, device_id=across(b), device_id_type=MESH)

    def block(i, owner):
        return grad_ref.at[0, pl.ds(pl.multiple_of(i * CHUNK, CHUNK), CHUNK), pl.ds(pl.multiple_of(owner * cols, cols), cols)]

    def at_rows(ref, i):
        return ref.at[pl.ds(pl.multiple_of(i * CHUNK, CHUNK), CHUNK)]

    def local_copy(which, i):
        owner, dst = ((far, fwd_own), (t, sum_own))[which]
        return pltpu.make_async_copy(block(i, owner), at_rows(dst, i), local_sem.at[which, i])

    def mate_copy(which, i):
        owner, dst = ((far_mate, fwd_mate), (mate, sum_mate))[which]
        return pltpu.make_async_remote_copy(
            src_ref=block(i, owner),
            dst_ref=at_rows(dst, i),
            send_sem=mate_send_sem.at[which, i],
            recv_sem=mate_recv_sem.at[which, i],
            device_id={"tp": mate},
            device_id_type=MESH,
        )

    def far_copy(i):
        return pltpu.make_async_remote_copy(
            src_ref=at_rows(fwd_send, i),
            dst_ref=at_rows(sum_far, i),
            send_sem=far_send_sem.at[i],
            recv_sem=far_recv_sem.at[i],
            device_id={"tp": far},
            device_id_type=MESH,
        )

    def hid_copy(k):
        q = lax.rem(p + k, ngroup)
        return pltpu.make_async_remote_copy(
            src_ref=hidden_ref.at[:, :, pl.ds(pl.multiple_of(q * rows, 128), rows)],
            dst_ref=hidden_in_v.at[k],
            send_sem=hid_send_sem.at[k - 1],
            recv_sem=hid_recv_sem.at[k - 1],
            device_id=group_id(k),
            device_id_type=MESH,
        )

    def sq_copy(k):
        return pltpu.make_async_remote_copy(
            src_ref=squares_send,
            dst_ref=squares_all.at[k],
            send_sem=sq_send_sem.at[k],
            recv_sem=sq_recv_sem.at[k],
            device_id=flat_id(k),
            device_id_type=MESH,
        )

    def proj_copy(k):
        return pltpu.make_async_remote_copy(
            src_ref=proj_send.at[k - 1],
            dst_ref=proj_recv.at[k - 1],
            send_sem=proj_send_sem.at[k - 1],
            recv_sem=proj_recv_sem.at[k - 1],
            device_id=group_id(ngroup - k),
            device_id_type=MESH,
        )

    def each(count, fn, start=0):
        def step(i, carry):
            fn(i)
            return carry

        lax.fori_loop(start, count, step, 0)

    each(nchunk, lambda i: local_copy(0, i).start())
    small = [
        pltpu.make_async_copy(src, dst, small_sem.at[i])
        for i, (src, dst) in enumerate(
            (
                (lengths_ref, lengths_s),
                (queries_ref, queries_v),
                (hidden_ref.at[:, :, pl.ds(pl.multiple_of(p * rows, 128), rows)], hidden_in_v.at[0]),
            )
        )
    ]
    for copy in small:
        copy.start()

    pl.semaphore_wait(barrier, bits)

    each(nchunk, lambda i: mate_copy(0, i).start())
    each(nchunk, lambda i: mate_copy(1, i).start())
    keys_copies = [pltpu.make_async_copy(keys_ref.at[i], keys_v.at[i], cache_sem.at[0, i]) for i in range(nrow)]
    values_copies = [pltpu.make_async_copy(values_ref.at[i], values_v.at[i], cache_sem.at[1, i]) for i in range(nrow)]
    for i in range(nrow):
        keys_copies[i].start()
        values_copies[i].start()
    each(nchunk, lambda i: local_copy(1, i).start())
    loads = [
        pltpu.make_async_copy(src, dst, load_sem.at[i])
        for i, (src, dst) in enumerate(((master_ref, master_v), (one_ref, one_v), (two_ref, two_v)))
    ]
    for copy in loads:
        copy.start()

    for copy in small:
        copy.wait()
    query_f[...] = jnp.zeros_like(query_f)
    for i in range(nrow):
        row_q = queries_v[i].astype(jnp.float32)
        for a in range(heads):
            for j in range(groups):
                n = a * groups + j
                query_f[a, i * PAD + j * nstep : i * PAD + (j + 1) * nstep, :] = row_q[:, n * HD : (n + 1) * HD]

    def forward(i):
        local_copy(0, i).wait()
        mate_copy(0, i).wait_recv()
        at_rows(fwd_send, i)[...] = (at_rows(fwd_own, i)[...] + at_rows(fwd_mate, i)[...]).astype(jnp.bfloat16)
        far_copy(i).start()

    for b in range(bits):
        pl.semaphore_signal(round_sem.at[b], inc=1, device_id=across(b), device_id_type=MESH)
        each((b + 1) * nchunk // bits, forward, b * nchunk // bits)
        pl.semaphore_wait(round_sem.at[b], 1)
    for k in range(1, ngroup):
        hid_copy(k).start()

    slot = lax.broadcasted_iota(jnp.int32, (PAD, slots), 1)
    for i in range(nrow):
        keys_copies[i].wait()
        values_copies[i].wait()
        valid = slot < lengths_s[i]
        for a in range(heads):
            q = query_f[a, i * PAD : (i + 1) * PAD, :].astype(jnp.bfloat16)
            scores = lax.dot_general(
                q,
                keys_v[i, :, a * HD : (a + 1) * HD],
                (((1,), (1,)), ((), ())),
                preferred_element_type=jnp.float32,
            )
            scores = jnp.where(valid, scores * scaling, NEG_FILL)
            top = jnp.max(scores, -1, keepdims=True)
            e = jnp.exp(scores - top)
            here = slice(i * PAD, (i + 1) * PAD)
            old_max[a, here, :] = jnp.broadcast_to(top, (PAD, HD))
            old_sum[a, here, :] = jnp.broadcast_to(jnp.sum(e, -1, keepdims=True), (PAD, HD))
            old_out[a, here, :] = jnp.dot(
                e.astype(jnp.bfloat16), values_v[i, :, a * HD : (a + 1) * HD], preferred_element_type=jnp.float32
            )

    for k in range(ngroup):
        if k > 0:
            hid_copy(k).wait_recv()
        own = hidden_in_v[k]
        for i in range(nrow):
            at = k * tokens + i * nstep
            hidden_f[at : at + nstep, :] = own[i].astype(jnp.float32)

    token = lax.broadcasted_iota(jnp.int32, (tokens, HD), 0)
    lane = lax.broadcasted_iota(jnp.int32, (tokens, HD), 1)
    position = lax.rem(token, nstep)
    for i in range(nrow):
        position = position + jnp.where(token // nstep == i, lengths_s[i], 0)
    pair = lax.rem(lane, HD // 2).astype(jnp.float32)
    angle = position.astype(jnp.float32) * jnp.exp(-math.log(ROPE_BASE) * 2.0 * pair / HD)
    cos_out[...] = jnp.cos(angle)
    sin_out[...] = jnp.where(lane < HD // 2, -jnp.sin(angle), jnp.sin(angle))

    def total(i, acc):
        local_copy(1, i).wait()
        mate_copy(1, i).wait_recv()
        far_copy(i).wait_recv()
        s = at_rows(sum_own, i)[...] + at_rows(sum_mate, i)[...] + at_rows(sum_far, i)[...].astype(jnp.float32)
        at_rows(grad_total, i)[...] = s
        return acc + jnp.sum((s * s).reshape(CHUNK // 8, 8, cols), axis=0)

    acc = lax.fori_loop(0, nchunk, total, jnp.zeros((8, cols), jnp.float32))
    part = jnp.sum(acc, axis=0, keepdims=True)
    mine = sum(part[:, j * 128 : (j + 1) * 128] for j in range(cols // 128))
    squares_send[...] = mine
    each(ndev, lambda k: sq_copy(k).start(), 1)
    squares_all[0] = mine
    for copy in loads:
        copy.wait()
    each(ndev, lambda k: sq_copy(k).wait_recv(), 1)
    squares = jnp.sum(jnp.sum(squares_all[...], axis=0), axis=1, keepdims=True)
    norm_limit = math.sqrt(D * 2 * KVH * HD)
    factor = jnp.minimum(1.0, norm_limit / jnp.sqrt(jnp.broadcast_to(squares, (1, cols))))

    def adam(i):
        clipped = at_rows(grad_total, i)[...] * factor
        one = BETA_ONE * at_rows(one_v, i)[...] + (1.0 - BETA_ONE) * clipped
        two = BETA_TWO * at_rows(two_v, i)[...] + (1.0 - BETA_TWO) * clipped * clipped
        at_rows(one_out, i)[...] = one
        at_rows(two_out, i)[...] = two
        update = (one * (LEARN_RATE / FIRST_CORR)) / (jnp.sqrt(two * (1.0 / SECOND_CORR)) + EPSILON)
        at_rows(weights_v, i)[...] = (at_rows(master_v, i)[...] - update).astype(jnp.bfloat16)

    each(nchunk, adam)
    partial = jnp.dot(hidden_f[...].astype(jnp.bfloat16), weights_v[...], preferred_element_type=jnp.float32)
    for k in range(1, ngroup):
        proj_send[k - 1] = partial[k * tokens : (k + 1) * tokens].astype(jnp.bfloat16)
        proj_copy(k).start()
    proj_own[...] = partial[0:tokens]

    each(nchunk, lambda i: mate_copy(0, i).wait_send())
    each(nchunk, lambda i: mate_copy(1, i).wait_send())
    each(nchunk, lambda i: far_copy(i).wait_send())
    each(ndev, lambda k: sq_copy(k).wait_send(), 1)
    for k in range(1, ngroup):
        hid_copy(k).wait_send()

    projected = proj_own[...]
    for k in range(1, ngroup):
        proj_copy(k).wait_recv()
        projected = projected + proj_recv[k - 1].astype(jnp.float32)
    proj_out[...] = projected
    for k in range(1, ngroup):
        proj_copy(k).wait_send()


def finish_kernel(
    one_ref,
    two_ref,
    proj_ref,
    cos_ref,
    sin_ref,
    query_ref,
    max_ref,
    sum_ref,
    old_ref,
    one_out,
    two_out,
    entries_out,
    attended_out,
    heads_v,
    out_sem,
):
    outs = [
        pltpu.make_async_copy(one_ref, one_out, out_sem.at[0]),
        pltpu.make_async_copy(two_ref, two_out, out_sem.at[1]),
    ]
    for copy in outs:
        copy.start()
    nrow, nstep, cols = entries_out.shape
    tokens = nrow * nstep
    heads = cols // (2 * HD)
    groups = QH // KVH
    scaling = 1.0 / math.sqrt(HD)
    qi = lax.broadcasted_iota(jnp.int32, (nrow * PAD, tokens), 0)
    kj = lax.broadcasted_iota(jnp.int32, (nrow * PAD, tokens), 1)
    seen = (qi // PAD == kj // nstep) & (qi % nstep >= kj % nstep)
    for a in range(heads):
        k = proj_ref[:, 2 * a * HD : (2 * a + 1) * HD]
        k = k * cos_ref[...] + pltpu.roll(k, HD // 2, 1) * sin_ref[...]
        v = proj_ref[:, (2 * a + 1) * HD : (2 * a + 2) * HD]
        new_k = k.astype(jnp.bfloat16)
        new_v = v.astype(jnp.bfloat16)
        for i in range(nrow):
            rows_i = slice(i * nstep, (i + 1) * nstep)
            entries_out[i, :, 2 * a * HD : (2 * a + 1) * HD] = k[rows_i].astype(jnp.bfloat16)
            entries_out[i, :, (2 * a + 1) * HD : (2 * a + 2) * HD] = v[rows_i].astype(jnp.bfloat16)
        scores = lax.dot_general(
            query_ref[a].astype(jnp.bfloat16), new_k, (((1,), (1,)), ((), ())), preferred_element_type=jnp.float32
        )
        scores = jnp.where(seen, scores * scaling, NEG_FILL)
        before = max_ref[a][:, 0:1]
        top = jnp.maximum(before, jnp.max(scores, -1, keepdims=True))
        alpha = jnp.exp(before - top)
        e = jnp.exp(scores - top)
        whole = sum_ref[a][:, 0:1] * alpha + jnp.sum(e, -1, keepdims=True)
        o = old_ref[a] * alpha + jnp.dot(e.astype(jnp.bfloat16), new_v, preferred_element_type=jnp.float32)
        heads_v[a] = o / whole
        for i in range(nrow):
            for j in range(groups):
                n = a * groups + j
                at = i * PAD + j * nstep
                attended_out[i, :, n * HD : (n + 1) * HD] = heads_v[a, at : at + nstep, :].astype(jnp.bfloat16)
    for copy in outs:
        copy.wait()


def fused_body(
    sizes,
    grad_parts,
    master,
    moment_one,
    moment_two,
    hidden_in,
    queries,
    cache_keys,
    cache_values,
    cache_lengths,
):
    ngrp, nrep, ntp = sizes
    ngroup = ngrp * nrep
    ndev = ngroup * ntp
    rows, cols = master.shape
    nrow, nstep, width = hidden_in.shape
    tokens = nrow * nstep
    heads = cols // (2 * HD)
    nchunk = rows // CHUNK
    f32, bf16 = jnp.float32, jnp.bfloat16
    vm = pltpu.VMEM
    dma = pltpu.SemaphoreType.DMA
    vmem = pl.BlockSpec(memory_space=pltpu.VMEM)
    hbm = pl.BlockSpec(memory_space=pltpu.HBM)
    per_head = vm((heads, nrow * PAD, HD), f32)
    moment = vm((rows, cols), f32)
    table = vm((tokens, HD), f32)
    middle = pl.pallas_call(
        functools.partial(fused_kernel, sizes),
        out_shape=(moment, moment, vm((tokens, cols), f32), table, table) + (per_head,) * 4,
        in_specs=[hbm] * 9,
        out_specs=(vmem,) * 9,
        scratch_shapes=[
            pltpu.SMEM((nrow,), jnp.int32),
            vm(queries.shape, bf16),
            vm((rows, cols), f32),
            vm((rows, cols), f32),
            vm((rows, cols), f32),
            vm((rows, cols), f32),
            vm((rows, cols), bf16),
            vm((rows, cols), bf16),
            vm((rows, cols), f32),
            vm((rows, cols), f32),
            vm((rows, cols), f32),
            vm((rows, cols), f32),
            vm(cache_keys.shape, bf16),
            vm(cache_values.shape, bf16),
            vm((ngroup, nrow, nstep, rows), bf16),
            vm((ngroup * tokens, rows), f32),
            vm((rows, cols), bf16),
            vm((1, 128), f32),
            vm((ndev, 1, 128), f32),
            vm((tokens, cols), f32),
            vm((ngroup - 1, tokens, cols), bf16),
            vm((ngroup - 1, tokens, cols), bf16),
            dma((2, nchunk)),
            dma((2, nchunk)),
            dma((2, nchunk)),
            dma((nchunk,)),
            dma((nchunk,)),
            dma((ngroup - 1,)),
            dma((ngroup - 1,)),
            dma((ndev,)),
            dma((ndev,)),
            dma((ngroup - 1,)),
            dma((ngroup - 1,)),
            dma((3,)),
            dma((2, nrow)),
            dma((3,)),
            pltpu.SemaphoreType.REGULAR((ndev.bit_length() - 1,)),
        ],
        compiler_params=pltpu.CompilerParams(
            collective_id=0, has_side_effects=True, vmem_limit_bytes=60 * 1024 * 1024 + 320 * 1024
        ),
    )(cache_lengths, hidden_in, queries, grad_parts, master, moment_one, moment_two, cache_keys, cache_values)
    return pl.pallas_call(
        finish_kernel,
        out_shape=(
            jax.ShapeDtypeStruct((rows, cols), f32),
            jax.ShapeDtypeStruct((rows, cols), f32),
            jax.ShapeDtypeStruct((nrow, nstep, cols), bf16),
            jax.ShapeDtypeStruct(queries.shape, bf16),
        ),
        in_specs=[vmem] * 9,
        out_specs=(hbm, hbm, vmem, vmem),
        scratch_shapes=[vm((heads, nrow * PAD, HD), f32), dma((2,))],
        compiler_params=pltpu.CompilerParams(vmem_limit_bytes=8 * 1024 * 1024),
    )(*middle)


def solution(mesh):
    sizes = (mesh.shape["grp"], mesh.shape["rep"], mesh.shape["tp"])
    fits = sizes[2] == 4 and D % (sizes[0] * sizes[1] * 128) == 0 and KVH % sizes[2] == 0
    fits = fits and (sizes[0] * sizes[1]) & (sizes[0] * sizes[1] - 1) == 0
    placed = (
        P("tp", ("grp", "rep"), None),
        P(("grp", "rep"), "tp"),
        P(("grp", "rep"), "tp"),
        P(("grp", "rep"), "tp"),
        P(("grp", "rep"), None, None),
        P(("grp", "rep"), None, "tp"),
        P(("grp", "rep"), None, "tp"),
        P(("grp", "rep"), None, "tp"),
        P(("grp", "rep")),
    )
    return jax.shard_map(
        functools.partial(fused_body, sizes) if fits else body,
        mesh=mesh,
        in_specs=placed,
        out_specs=(
            P(("grp", "rep"), "tp"),
            P(("grp", "rep"), "tp"),
            P(("grp", "rep"), None, "tp"),
            P(("grp", "rep"), None, "tp"),
        ),
        check_vma=False,
    )
```
